128 devices in a mesh: row: 8 (over y_hi, z), col: 16 (over x, y_lo, core).
Axes of the slice: x: 4, y: 4 (y_hi: 2, y_lo: 2; y = y_hi * 2 + y_lo), z: 4, core: 2. Of those that a mesh axis runs over, the one named last changes fastest.
Arguments:
- response_coeffs: float32 [3, 8192, 1024], P(None, ('row', 'col')), may hold values from -6 to 6
- occupied_coeffs: float32 [8192, 1024], P(('row', 'col')), may hold values from -0.1875 to 0.1875
Outputs:
- density: float32 [3, 8192, 8192], P(None, 'row', 'col')
The draws below stay inside these ranges and needn't reach their ends.
All inputs are finite; a program needn't handle non-finite values.
Results may differ from the reference program's by a relative error of at most 0.0003.
Values sent between devices are 32-bit elements; how exact they have to be, the bound alone decides.
A program may use at most 128 MiB of HBM per device.

```python
import jax
import jax.numpy as jnp
from jax import lax

BASIS = 8192
OCC = 1024
PERTURB = 3


def level_of(key, dims, split, low, top_value):
    gain, own = 1.0, jax.random.fold_in(key, 6)
    for dim, blocks in split:
        heights = jnp.exp(jax.random.uniform(jax.random.fold_in(own, dim), (blocks,), jnp.float32, low / len(split), top_value / len(split)))
        gain = gain * jnp.repeat(heights, dims[dim] // blocks).reshape([-1 if axis == dim else 1 for axis in range(len(dims))])
    return gain


def normal_values(rng, shape, deviation, most, pieces=(), dtype=jnp.bfloat16):
    values = deviation * jax.random.normal(rng, shape, jnp.float32)
    if pieces:
        values = values * level_of(rng, shape, pieces, -0.22, 0.18)
    return jnp.clip(values, -most, most).astype(dtype)


def setup_inputs(seed: int = 0) -> dict:
    keys = jax.random.split(jax.random.key(seed), 3)
    response_coeffs = normal_values(keys[0], (PERTURB, BASIS, OCC), 1.0, 6.0, ((1, 128),), jnp.float32)
    occupied_coeffs = normal_values(keys[1], (BASIS, OCC), OCC ** -0.5, 0.1875, ((0, 128),), jnp.float32)
    return dict(response_coeffs=response_coeffs, occupied_coeffs=occupied_coeffs)


SLICE_PAIRS = ((0, 0), (0, 1), (1, 0))


def split_slices(values):
    leading = lax.optimization_barrier(values.astype(jnp.bfloat16))
    remainder = values - leading.astype(jnp.float32)
    trailing = lax.optimization_barrier(remainder.astype(jnp.bfloat16))
    return [leading, trailing]


def reference(response_coeffs, occupied_coeffs):
    response_slices = split_slices(response_coeffs)
    occupied_slices = split_slices(occupied_coeffs)
    accumulated = jnp.zeros((PERTURB, BASIS, BASIS), jnp.float32)
    for left_index, right_index in SLICE_PAIRS:
        accumulated = accumulated + jnp.einsum(
            "kno,mo->knm",
            response_slices[left_index].astype(jnp.float32),
            occupied_slices[right_index].astype(jnp.float32),
            precision=lax.Precision.HIGHEST,
        )
    return accumulated + jnp.swapaxes(accumulated, 1, 2)
```

```python
import functools

import jax
import jax.numpy as jnp
from jax import lax
from jax.experimental import pallas as pl
from jax.experimental.pallas import tpu as pltpu
from jax.sharding import PartitionSpec as P

MESH = pl.DeviceIdType.MESH
CHUNKS = 8
ROW_SHARDS = 16
COLUMN_SHARDS = 8
SHARDS = ROW_SHARDS + COLUMN_SHARDS

FROM_LEFT, FROM_RIGHT, FROM_PAIR = 0, 1, 2
LEFT_FAR, RIGHT_FAR = 3, 4
PAIR_LEFT, PAIR_RIGHT = 5, 6
PAIR_LEFT_FAR, PAIR_RIGHT_FAR = 7, 8
PLANE_EVENTS = 9
ROW_BASE = 0
COLUMN_BASE = PLANE_EVENTS
CORE_BASE = 2 * PLANE_EVENTS
CORE_OWN = CORE_BASE + PLANE_EVENTS
TURNED = CORE_OWN + 1
EVENTS = TURNED + 1


def kernel(response_ref, occupied_ref, density_ref, land, high, low, total, load_sem, send_sem, recv_sem, out_sem):
    perturbations, rows, occupied = response_ref.shape
    chunks, _, arrays, _, depth = land.shape
    row, col = lax.axis_index("row"), lax.axis_index("col")
    h, z = row // 4, row % 4
    x, l, c = col // 4, (col // 2) % 2, col % 2

    def device(h_, z_, x_, l_, c_):
        return (h_ * 4 + z_, x_ * 4 + l_ * 2 + c_)

    right, left = device(h, z, (x + 1) % 4, l, c), device(h, z, (x + 3) % 4, l, c)
    near = device(h, z, x, 1 - l, c)
    up, down = device(h, (z + 1) % 4, x, l, c), device(h, (z + 3) % 4, x, l, c)
    across = device(1 - h, z, x, l, c)
    twin = device(h, z, x, l, 1 - c)
    turned_h = (h + x + jnp.where(row == 0, 1, 0)) % 2
    turn_to = (turned_h * 4 + (z + col % 4) % 4, row * 2 + col // 8)
    group = col // 2
    source_h, source_z = group // 4, group % 4
    odd = jnp.where(group == 0, 1, 0)
    source_x = 2 * c + (h + source_h + odd) % 2
    turn_from = (group, source_x * 4 + (z + 4 - source_z) % 4)

    def row_slot(step, flip):
        return ((x + step) % 4) * 4 + ((l + flip) % 2) * 2 + c

    def column_slot(step, flip):
        return ROW_SHARDS + ((h + flip + source_h + odd) % 2) * 4 + (z + step + 4 - source_z) % 4

    barrier = pltpu.get_barrier_semaphore()
    peers = (right, left, near, up, down, across, twin, turn_to, turn_from)
    for peer in peers:
        pl.semaphore_signal(barrier, inc=1, device_id=peer, device_id_type=MESH)

    def load(chunk):
        columns = pl.ds(pl.multiple_of(chunk * depth, depth), depth)
        return (
            pltpu.make_async_copy(response_ref.at[:, :, columns], land.at[chunk, col, pl.ds(0, perturbations)], load_sem.at[chunk, 0]),
            pltpu.make_async_copy(occupied_ref.at[:, columns], land.at[chunk, col, perturbations], load_sem.at[chunk, 1]),
        )

    @pl.loop(0, chunks)
    def _(chunk):
        for copy in load(chunk):
            copy.start()

    def part(chunk, slot, half):
        if half is None:
            return land.at[chunk, slot]
        return land.at[chunk, slot, pl.ds(half * (arrays // 2), arrays // 2)]

    def transfer(chunk, source, slot, event, peer, half=None):
        return pltpu.make_async_remote_copy(
            src_ref=part(chunk, source, half),
            dst_ref=part(chunk, slot, half),
            send_sem=send_sem.at[chunk],
            recv_sem=recv_sem.at[chunk, event],
            device_id=peer,
            device_id_type=MESH,
        )

    def send(chunk, slot, event, peer, half=None):
        transfer(chunk, slot, slot, event, peer, half).start()

    def arrived(chunk, slot, event, half=None):
        transfer(chunk, slot, slot, event, twin, half).wait_recv()

    def begin(chunk):
        for copy in load(chunk):
            copy.wait()
        transfer(chunk, col, ROW_SHARDS + col % 8, TURNED, turn_to).start()
        send(chunk, col, ROW_BASE + FROM_LEFT, right)
        send(chunk, col, ROW_BASE + FROM_RIGHT, left)
        send(chunk, col, ROW_BASE + FROM_PAIR, near)
        send(chunk, col, CORE_OWN, twin)

    def turn(chunk):
        slot = column_slot(0, 0)
        arrived(chunk, slot, TURNED)
        send(chunk, slot, COLUMN_BASE + FROM_LEFT, up)
        send(chunk, slot, COLUMN_BASE + FROM_RIGHT, down)
        send(chunk, slot, COLUMN_BASE + FROM_PAIR, across)

    def relay(chunk, slot, base, event, forward, half=None):
        arrived(chunk, slot, base + event, half)
        for next_event, peer, next_half in forward:
            send(chunk, slot, base + next_event, peer, next_half)
        if base == ROW_BASE:
            send(chunk, slot, CORE_BASE + event, twin, half)

    def first(chunk):
        for base, slot, ahead, behind in ((ROW_BASE, row_slot, right, left), (COLUMN_BASE, column_slot, up, down)):
            relay(chunk, slot(3, 0), base, FROM_LEFT, ((LEFT_FAR, ahead, 0),))
            relay(chunk, slot(1, 0), base, FROM_RIGHT, ((RIGHT_FAR, behind, 1),))
            relay(chunk, slot(0, 1), base, FROM_PAIR, ((PAIR_LEFT, ahead, None), (PAIR_RIGHT, behind, None)))

    def second(chunk):
        for base, slot, ahead, behind in ((ROW_BASE, row_slot, right, left), (COLUMN_BASE, column_slot, up, down)):
            relay(chunk, slot(2, 0), base, LEFT_FAR, (), 0)
            relay(chunk, slot(2, 0), base, RIGHT_FAR, (), 1)
            relay(chunk, slot(3, 1), base, PAIR_LEFT, ((PAIR_LEFT_FAR, ahead, 0),))
            relay(chunk, slot(1, 1), base, PAIR_RIGHT, ((PAIR_RIGHT_FAR, behind, 1),))

    def third(chunk):
        for base, slot in ((ROW_BASE, row_slot), (COLUMN_BASE, column_slot)):
            relay(chunk, slot(2, 1), base, PAIR_LEFT_FAR, (), 0)
            relay(chunk, slot(2, 1), base, PAIR_RIGHT_FAR, (), 1)

    def other(step, flip):
        return ((x + step) % 4) * 4 + ((l + flip) % 2) * 2 + 1 - c

    def fourth(chunk):
        arrived(chunk, other(0, 0), CORE_OWN)
        arrived(chunk, other(3, 0), CORE_BASE + FROM_LEFT)
        arrived(chunk, other(1, 0), CORE_BASE + FROM_RIGHT)
        arrived(chunk, other(0, 1), CORE_BASE + FROM_PAIR)
        arrived(chunk, other(2, 0), CORE_BASE + LEFT_FAR, 0)
        arrived(chunk, other(2, 0), CORE_BASE + RIGHT_FAR, 1)
        arrived(chunk, other(3, 1), CORE_BASE + PAIR_LEFT)
        arrived(chunk, other(1, 1), CORE_BASE + PAIR_RIGHT)
        arrived(chunk, other(2, 1), CORE_BASE + PAIR_LEFT_FAR, 0)
        arrived(chunk, other(2, 1), CORE_BASE + PAIR_RIGHT_FAR, 1)

    def split(chunk):
        @pl.loop(0, SHARDS)
        def _(shard):
            values = land[chunk, shard]
            leading = values.astype(jnp.bfloat16)
            trailing = (values - leading.astype(jnp.float32)).astype(jnp.bfloat16)
            where = pl.ds(pl.multiple_of(shard * rows, rows), rows)
            high[:, where, :] = leading
            low[:, where, :] = trailing

    columns_out = COLUMN_SHARDS * rows
    rows_out = ROW_SHARDS * rows
    tile = 256

    def multiply(k):
        there = pl.ds(rows_out, columns_out)
        right_side = jnp.concatenate(
            [high[perturbations, there], low[perturbations, there], high[perturbations, there], high[k, there], high[k, there], low[k, there]], axis=1
        )

        @pl.loop(0, rows_out // tile)
        def _(m):
            here = pl.ds(pl.multiple_of(m * tile, tile), tile)
            left_side = jnp.concatenate(
                [high[k, here], high[k, here], low[k, here], high[perturbations, here], low[perturbations, here], high[perturbations, here]], axis=1
            )
            total[k, here, :] += lax.dot_general(
                left_side, right_side, (((1,), (1,)), ((), ())), preferred_element_type=jnp.float32
            )

    pl.semaphore_wait(barrier, len(peers))
    begin(0)
    begin(1)

    @pl.loop(0, perturbations)
    def _(k):
        total[k] = jnp.zeros(total.shape[1:], jnp.float32)

    turn(0)
    first(0)

    @pl.loop(0, chunks)
    def _(chunk):
        @pl.when(chunk + 2 < chunks)
        def _():
            begin(chunk + 2)

        @pl.when(chunk + 1 < chunks)
        def _():
            turn(chunk + 1)

        second(chunk)

        @pl.when(chunk + 1 < chunks)
        def _():
            first(chunk + 1)

        third(chunk)
        fourth(chunk)
        split(chunk)

        @pl.loop(0, perturbations)
        def _(k):
            multiply(k)

            @pl.when(chunk == chunks - 1)
            def _():
                pltpu.make_async_copy(total.at[k], density_ref.at[k], out_sem.at[k]).start()

    @pl.loop(0, chunks)
    def _(chunk):
        sent = land.at[chunk, pl.ds(0, SHARDS - 1)]
        pltpu.make_async_copy(sent, sent, send_sem.at[chunk]).wait()

    for k in range(perturbations):
        pltpu.make_async_copy(total.at[k], density_ref.at[k], out_sem.at[k]).wait()


def shards(response_coeffs, occupied_coeffs):
    perturbations, rows, occupied = response_coeffs.shape
    depth = occupied // CHUNKS
    return pl.pallas_call(
        kernel,
        name="gather_multiply",
        out_shape=jax.ShapeDtypeStruct((perturbations, ROW_SHARDS * rows, COLUMN_SHARDS * rows), jnp.float32),
        in_specs=[pl.BlockSpec(memory_space=pl.ANY)] * 2,
        out_specs=pl.BlockSpec(memory_space=pl.ANY),
        scratch_shapes=[
            pltpu.VMEM((CHUNKS, SHARDS, perturbations + 1, rows, depth), jnp.float32),
            pltpu.VMEM((perturbations + 1, SHARDS * rows, depth), jnp.bfloat16),
            pltpu.VMEM((perturbations + 1, SHARDS * rows, depth), jnp.bfloat16),
            pltpu.VMEM((perturbations, ROW_SHARDS * rows, COLUMN_SHARDS * rows), jnp.float32),
            pltpu.SemaphoreType.DMA((CHUNKS, 2)),
            pltpu.SemaphoreType.DMA((CHUNKS,)),
            pltpu.SemaphoreType.DMA((CHUNKS, EVENTS)),
            pltpu.SemaphoreType.DMA((perturbations,)),
        ],
        compiler_params=pltpu.CompilerParams(
            collective_id=0, has_side_effects=True, vmem_limit_bytes=56 * 1024 * 1024
        ),
    )(response_coeffs, occupied_coeffs)


def solution(mesh):
    return jax.shard_map(
        shards,
        mesh=mesh,
        in_specs=(P(None, ("row", "col"), None), P(("row", "col"), None)),
        out_specs=P(None, "row", "col"),
        check_vma=False,
    )
```

```python
import functools

import jax
import jax.numpy as jnp
from jax import lax
from jax.experimental import pallas as pl
from jax.experimental.pallas import tpu as pltpu
from jax.sharding import PartitionSpec as P

MESH = pl.DeviceIdType.MESH
CHUNKS = 8
ROW_SHARDS = 16
COLUMN_SHARDS = 8
SHARDS = ROW_SHARDS + COLUMN_SHARDS
TURN_SLOTS = 2

LEFT, RIGHT, PAIR, LEFT_FAR, RIGHT_FAR = 0, 1, 2, 3, 4
PAIR_LEFT, PAIR_RIGHT, PAIR_LEFT_FAR, PAIR_RIGHT_FAR = 5, 6, 7, 8
PLANE_EVENTS = 9
ROW_BASE = 0
COLUMN_BASE = PLANE_EVENTS
CORE_BASE = 2 * PLANE_EVENTS
CORE_OWN = 3 * PLANE_EVENTS
TURN_BASE = CORE_OWN + 1
EVENTS = TURN_BASE + 3


def kernel(response_ref, occupied_ref, density_ref, land, high, low, total, load_sem, send_sem, turn_sem, recv_sem, out_sem):
    perturbations, rows, occupied = response_ref.shape
    chunks, _, arrays, _, depth = land.shape
    row, col = lax.axis_index("row"), lax.axis_index("col")
    h, z = row // 4, row % 4
    x, l, c = col // 4, (col // 2) % 2, col % 2

    def device(h_, z_, x_, l_, c_):
        return (h_ * 4 + z_ % 4, (x_ % 4) * 4 + l_ * 2 + c_)

    def along_x(step):
        return device(h, z, x + step, l, c)

    def along_z(step):
        return device(h, z + step, x, l, c)

    near = device(h, z, x, 1 - l, c)
    across = device(1 - h, z, x, l, c)
    twin = device(h, z, x, l, 1 - c)

    def differs(a, b):
        return jnp.logical_or(a[0] != b[0], a[1] != b[1])

    here = device(h, z, x, l, c)
    offset = 2 * c + l
    moved_z = offset != 0
    z_mid = (z + 4 - offset) % 4
    to_y = device((h + x) % 2, z, x, z_mid % 2, c)
    l_y = (z + l) % 2
    z_y = (z + 8 - 2 * c - l_y) % 4
    h_y = (h + x) % 2
    from_y = device(h_y, z, x, l_y, c)
    to_x = device(h, z, h_y * 2 + z_y // 2, l, x // 2)
    h_s, z_s = x // 2, (x % 2) * 2 + l
    offset_s = (z + 4 - z_s) % 4
    x_s = c * 2 + (h + h_s) % 2
    from_x = device(h, z, x_s, l, offset_s // 2)
    goes_y, came_y = differs(here, to_y), differs(here, from_y)
    goes_x, came_x = differs(here, to_x), differs(here, from_x)

    def column_slot(step, flip):
        there = (z + step + 4 - z_s) % 4
        return ROW_SHARDS + ((h + flip + h_s) % 2) * 4 + (there % 2) * 2 + there // 2

    def row_slot(step, flip, core):
        return ((x + step) % 4) * 4 + ((l + flip) % 2) * 2 + core

    place_z = jnp.where(moved_z, SHARDS, col)
    place_y = jnp.where(came_y, SHARDS + 1, place_z)
    own_column = column_slot(0, 0)
    place_x = jnp.where(came_x, own_column, place_y)

    barrier = pltpu.get_barrier_semaphore()
    peers = [along_x(1), along_x(3), along_z(1), along_z(3), along_z(2)] + [near, across, twin]
    peers += [device(1 - h, z, x, 1 - l, c)] + [device(h, z, x + s, l, 1 - c) for s in (1, 2, 3)] + [along_x(2)]
    for peer in peers:
        pl.semaphore_signal(barrier, inc=1, device_id=peer, device_id_type=MESH)

    def load(chunk):
        columns = pl.ds(pl.multiple_of(chunk * depth, depth), depth)
        return (
            pltpu.make_async_copy(response_ref.at[:, :, columns], land.at[chunk, col, pl.ds(0, perturbations)], load_sem.at[chunk, 0]),
            pltpu.make_async_copy(occupied_ref.at[:, columns], land.at[chunk, col, perturbations], load_sem.at[chunk, 1]),
        )

    @pl.loop(0, chunks)
    def _(chunk):
        for copy in load(chunk):
            copy.start()

    def part(chunk, slot, half):
        if half is None:
            return land.at[chunk, slot]
        return land.at[chunk, slot, pl.ds(half * (arrays // 2), arrays // 2)]

    def transfer(chunk, source, slot, event, peer, sem=None, half=None):
        return pltpu.make_async_remote_copy(
            src_ref=part(chunk, source, half),
            dst_ref=part(chunk, slot, half),
            send_sem=send_sem.at[chunk] if sem is None else sem,
            recv_sem=recv_sem.at[chunk, event],
            device_id=peer,
            device_id_type=MESH,
        )

    def send(chunk, source, slot, event, peer, half=None):
        transfer(chunk, source, slot, event, peer, None, half).start()

    def arrived(chunk, slot, event, half=None):
        transfer(chunk, slot, slot, event, twin, None, half).wait_recv()

    def turn_z(chunk):
        return transfer(chunk, col, SHARDS, TURN_BASE, along_z(offset), turn_sem.at[chunk, 0])

    def turn_y(chunk):
        return transfer(chunk, place_z, SHARDS + 1, TURN_BASE + 1, to_y, turn_sem.at[chunk, 1])

    def turn_x(chunk):
        x_to, c_to = h_y * 2 + z_y // 2, x // 2
        slot = ROW_SHARDS + (x % 2) * 4 + l_y * 2 + c
        return transfer(chunk, place_y, slot, TURN_BASE + 2, to_x, turn_sem.at[chunk, 2])

    def begin(chunk):
        send(chunk, col, col, ROW_BASE + PAIR, near)
        send(chunk, col, col, ROW_BASE + LEFT, along_x(1))
        send(chunk, col, col, ROW_BASE + RIGHT, along_x(3))
        send(chunk, col, col, CORE_OWN, twin)

    def turn_first(chunk):
        for copy in load(chunk):
            copy.wait()

        @pl.when(moved_z)
        def _():
            turn_z(chunk).start()

    def turn_second(chunk):
        @pl.when(moved_z)
        def _():
            turn_z(chunk).wait_recv()

        @pl.when(goes_y)
        def _():
            turn_y(chunk).start()

    def turn_third(chunk):
        @pl.when(came_y)
        def _():
            turn_y(chunk).wait_recv()

        @pl.when(goes_x)
        def _():
            turn_x(chunk).start()

    def turned(chunk):
        @pl.when(came_x)
        def _():
            arrived(chunk, own_column, TURN_BASE + 2)

        send(chunk, place_x, own_column, COLUMN_BASE + PAIR, across)
        send(chunk, place_x, own_column, COLUMN_BASE + LEFT, along_z(1))
        send(chunk, place_x, own_column, COLUMN_BASE + RIGHT, along_z(3))

    def relay(chunk, slot, base, event, forward, half=None):
        arrived(chunk, slot, base + event, half)
        for next_event, peer, next_half in forward:
            send(chunk, slot, slot, base + next_event, peer, next_half)
        if base == ROW_BASE:
            send(chunk, slot, slot, CORE_BASE + event, twin, half)

    def row_place(step, flip):
        return row_slot(step, flip, c)

    planes = ((ROW_BASE, row_place, along_x), (COLUMN_BASE, column_slot, along_z))

    def first(plane, chunk):
        base, slot, along = plane
        relay(chunk, slot(0, 1), base, PAIR, ((PAIR_LEFT, along(1), None), (PAIR_RIGHT, along(3), None)))
        relay(chunk, slot(3, 0), base, LEFT, ((LEFT_FAR, along(1), 0),))
        relay(chunk, slot(1, 0), base, RIGHT, ((RIGHT_FAR, along(3), 1),))

    def second(plane, chunk):
        base, slot, along = plane
        relay(chunk, slot(3, 1), base, PAIR_LEFT, ((PAIR_LEFT_FAR, along(1), 0),))
        relay(chunk, slot(1, 1), base, PAIR_RIGHT, ((PAIR_RIGHT_FAR, along(3), 1),))
        relay(chunk, slot(2, 0), base, LEFT_FAR, (), 0)
        relay(chunk, slot(2, 0), base, RIGHT_FAR, (), 1)

    def third(plane, chunk):
        base, slot, along = plane
        relay(chunk, slot(2, 1), base, PAIR_LEFT_FAR, (), 0)
        relay(chunk, slot(2, 1), base, PAIR_RIGHT_FAR, (), 1)

    row_first, column_first = functools.partial(first, planes[0]), functools.partial(first, planes[1])
    row_second, column_second = functools.partial(second, planes[0]), functools.partial(second, planes[1])
    row_third, column_third = functools.partial(third, planes[0]), functools.partial(third, planes[1])

    def from_twin(chunk):
        arrived(chunk, row_slot(0, 0, 1 - c), CORE_OWN)
        for step, flip, event, half in (
            (0, 1, PAIR, None), (3, 0, LEFT, None), (1, 0, RIGHT, None), (3, 1, PAIR_LEFT, None), (1, 1, PAIR_RIGHT, None),
            (2, 0, LEFT_FAR, 0), (2, 0, RIGHT_FAR, 1), (2, 1, PAIR_LEFT_FAR, 0), (2, 1, PAIR_RIGHT_FAR, 1),
        ):
            arrived(chunk, row_slot(step, flip, 1 - c), CORE_BASE + event, half)

    def split(chunk):
        @pl.loop(0, SHARDS)
        def _(shard):
            values = land[chunk, jnp.where(shard == own_column, place_x, shard)]
            leading = values.astype(jnp.bfloat16)
            trailing = (values - leading.astype(jnp.float32)).astype(jnp.bfloat16)
            where = pl.ds(pl.multiple_of(shard * rows, rows), rows)
            high[:, where, :] = leading
            low[:, where, :] = trailing

    rows_out = ROW_SHARDS * rows

    def multiply(k):
        ours, theirs = slice(0, rows_out), slice(rows_out, SHARDS * rows)
        o = perturbations
        left_side = jnp.concatenate(
            [high[k, ours], high[k, ours], low[k, ours], high[o, ours], low[o, ours], high[o, ours]], axis=1
        )
        right_side = jnp.concatenate(
            [high[o, theirs], low[o, theirs], high[o, theirs], high[k, theirs], high[k, theirs], low[k, theirs]], axis=1
        )
        total[k] += lax.dot_general(
            left_side, right_side, (((1,), (1,)), ((), ())), preferred_element_type=jnp.float32
        )

    def ahead(chunk, step):
        pl.when(chunk < chunks)(lambda: step(chunk))

    pl.semaphore_wait(barrier, len(peers))
    for chunk in range(3):
        turn_first(chunk)
    begin(0)

    @pl.loop(3, chunks)
    def _(chunk):
        turn_first(chunk)

    turn_second(0)
    turn_second(1)
    begin(1)
    turn_second(2)
    turn_third(0)
    row_first(0)
    turn_second(3)
    turn_third(1)
    turned(0)
    begin(2)

    @pl.loop(0, perturbations)
    def _(k):
        total[k] = jnp.zeros(total.shape[1:], jnp.float32)

    row_second(0)
    row_first(1)
    turn_second(4)
    turn_third(2)
    turned(1)
    column_first(0)
    turn_second(5)
    turn_third(3)
    turned(2)
    column_second(0)
    column_first(1)

    @pl.loop(0, chunks)
    def _(chunk):
        ahead(chunk + 1, row_second)
        ahead(chunk + 2, row_first)
        ahead(chunk + 3, begin)
        ahead(chunk + 6, turn_second)
        ahead(chunk + 4, turn_third)
        ahead(chunk + 3, turned)
        ahead(chunk + 1, column_second)
        ahead(chunk + 2, column_first)
        row_third(chunk)
        column_third(chunk)
        from_twin(chunk)
        split(chunk)

        @pl.loop(0, perturbations)
        def _(k):
            multiply(k)

            @pl.when(chunk == chunks - 1)
            def _():
                pltpu.make_async_copy(total.at[k], density_ref.at[k], out_sem.at[k]).start()

    @pl.loop(0, chunks)
    def _(chunk):
        sent = land.at[chunk, pl.ds(0, 22)]
        pltpu.make_async_copy(sent, sent, send_sem.at[chunk]).wait()
        pl.when(moved_z)(lambda: turn_z(chunk).wait_send())
        pl.when(goes_y)(lambda: turn_y(chunk).wait_send())
        pl.when(goes_x)(lambda: turn_x(chunk).wait_send())

    for k in range(perturbations):
        pltpu.make_async_copy(total.at[k], density_ref.at[k], out_sem.at[k]).wait()


def shards(response_coeffs, occupied_coeffs):
    perturbations, rows, occupied = response_coeffs.shape
    depth = occupied // CHUNKS
    return pl.pallas_call(
        kernel,
        name="gather_multiply",
        out_shape=jax.ShapeDtypeStruct((perturbations, ROW_SHARDS * rows, COLUMN_SHARDS * rows), jnp.float32),
        in_specs=[pl.BlockSpec(memory_space=pl.ANY)] * 2,
        out_specs=pl.BlockSpec(memory_space=pl.ANY),
        scratch_shapes=[
            pltpu.VMEM((CHUNKS, SHARDS + TURN_SLOTS, perturbations + 1, rows, depth), jnp.float32),
            pltpu.VMEM((perturbations + 1, SHARDS * rows, depth), jnp.bfloat16),
            pltpu.VMEM((perturbations + 1, SHARDS * rows, depth), jnp.bfloat16),
            pltpu.VMEM((perturbations, ROW_SHARDS * rows, COLUMN_SHARDS * rows), jnp.float32),
            pltpu.SemaphoreType.DMA((CHUNKS, 2)),
            pltpu.SemaphoreType.DMA((CHUNKS,)),
            pltpu.SemaphoreType.DMA((CHUNKS, 3)),
            pltpu.SemaphoreType.DMA((CHUNKS, EVENTS)),
            pltpu.SemaphoreType.DMA((perturbations,)),
        ],
        compiler_params=pltpu.CompilerParams(
            collective_id=0, has_side_effects=True, vmem_limit_bytes=56 * 1024 * 1024
        ),
    )(response_coeffs, occupied_coeffs)


def solution(mesh):
    return jax.shard_map(
        shards,
        mesh=mesh,
        in_specs=(P(None, ("row", "col"), None), P(("row", "col"), None)),
        out_specs=P(None, "row", "col"),
        check_vma=False,
    )
```

```python
import functools

import jax
import jax.numpy as jnp
from jax import lax
from jax.experimental import pallas as pl
from jax.experimental.pallas import tpu as pltpu
from jax.sharding import PartitionSpec as P

MESH = pl.DeviceIdType.MESH
CHUNKS = 8
ROW_SHARDS = 16
COLUMN_SHARDS = 8
SHARDS = ROW_SHARDS + COLUMN_SHARDS
TURN_SLOTS = 2

LEFT, RIGHT, PAIR, LEFT_FAR, RIGHT_FAR = 0, 1, 2, 3, 4
PAIR_LEFT, PAIR_RIGHT, PAIR_LEFT_FAR, PAIR_RIGHT_FAR = 5, 6, 7, 8
PLANE_EVENTS = 9
ROW_BASE = 0
COLUMN_BASE = PLANE_EVENTS
CORE_BASE = 2 * PLANE_EVENTS
CORE_OWN = 3 * PLANE_EVENTS
TURN_BASE = CORE_OWN + 1
EVENTS = TURN_BASE + 3


def kernel(response_ref, occupied_ref, high, low, total, land, load_sem, send_sem, turn_sem, recv_sem):
    perturbations, rows, occupied = response_ref.shape
    chunks, _, arrays, _, depth = land.shape
    row, col = lax.axis_index("row"), lax.axis_index("col")
    h, z = row // 4, row % 4
    x, l, c = col // 4, (col // 2) % 2, col % 2

    def device(h_, z_, x_, l_, c_):
        return (h_ * 4 + z_ % 4, (x_ % 4) * 4 + l_ * 2 + c_)

    def along_x(step):
        return device(h, z, x + step, l, c)

    def along_z(step):
        return device(h, z + step, x, l, c)

    near = device(h, z, x, 1 - l, c)
    across = device(1 - h, z, x, l, c)
    twin = device(h, z, x, l, 1 - c)

    def differs(a, b):
        return jnp.logical_or(a[0] != b[0], a[1] != b[1])

    here = device(h, z, x, l, c)
    h_s, z_s = x // 2, (x % 2) * 2 + l

    def route(chunk):
        odd = chunk % 2
        offset = (2 * c + l + 2 * odd) % 4
        to_y = device((h + x + odd) % 2, z, x, (z + offset) % 2, c)
        l_y = (z + l) % 2
        z_y = (z + 8 - 2 * c - l_y - 2 * odd) % 4
        h_y = (h + x + odd) % 2
        from_y = device(h_y, z, x, l_y, c)
        to_x = device(h, z, h_y * 2 + z_y // 2, l, x // 2)
        from_x = device(h, z, c * 2 + (h + h_s + odd) % 2, l, (z + 8 - z_s - 2 * odd) % 4 // 2)
        moved_z, came_y, came_x = offset != 0, differs(here, from_y), differs(here, from_x)
        goes_y, goes_x = differs(here, to_y), differs(here, to_x)
        place_z = jnp.where(moved_z, SHARDS, col)
        place_y = jnp.where(came_y, SHARDS + 1, place_z)
        place_x = jnp.where(came_x, column_slot(chunk, 0, 0), place_y)
        slot_x = ROW_SHARDS + (x % 2) * 4 + l_y * 2 + c
        return offset, to_y, to_x, moved_z, goes_y, came_y, goes_x, came_x, place_z, place_y, place_x, slot_x

    def column_slot(chunk, step, flip):
        odd = chunk % 2
        there = (z + step + 8 - z_s - 2 * odd) % 4
        return ROW_SHARDS + ((h + flip + h_s + odd) % 2) * 4 + (there % 2) * 2 + there // 2

    def row_slot(step, flip, core):
        return ((x + step) % 4) * 4 + ((l + flip) % 2) * 2 + core

    barrier = pltpu.get_barrier_semaphore()
    peers = [along_x(1), along_x(3), along_z(1), along_z(3), along_z(2)] + [near, across, twin]
    peers += [device(1 - h, z, x, 1 - l, c)] + [device(h, z, x + s, l, 1 - c) for s in (1, 2, 3)] + [along_x(2)]
    for peer in peers:
        pl.semaphore_signal(barrier, inc=1, device_id=peer, device_id_type=MESH)

    def load(chunk):
        columns = pl.ds(pl.multiple_of(chunk * depth, depth), depth)
        return (
            pltpu.make_async_copy(response_ref.at[:, :, columns], land.at[chunk, col, pl.ds(0, perturbations)], load_sem.at[chunk, 0]),
            pltpu.make_async_copy(occupied_ref.at[:, columns], land.at[chunk, col, perturbations], load_sem.at[chunk, 1]),
        )

    @pl.loop(0, chunks)
    def _(chunk):
        for copy in load(chunk):
            copy.start()

    def part(chunk, slot, half):
        if half is None:
            return land.at[chunk, slot]
        return land.at[chunk, slot, pl.ds(half * (arrays // 2), arrays // 2)]

    def transfer(chunk, source, slot, event, peer, sem=None, half=None):
        return pltpu.make_async_remote_copy(
            src_ref=part(chunk, source, half),
            dst_ref=part(chunk, slot, half),
            send_sem=send_sem.at[chunk] if sem is None else sem,
            recv_sem=recv_sem.at[chunk, event],
            device_id=peer,
            device_id_type=MESH,
        )

    def send(chunk, source, slot, event, peer, half=None):
        transfer(chunk, source, slot, event, peer, None, half).start()

    def arrived(chunk, slot, event, half=None):
        transfer(chunk, slot, slot, event, twin, None, half).wait_recv()

    def turn_z(chunk):
        offset = route(chunk)[0]
        return transfer(chunk, col, SHARDS, TURN_BASE, along_z(offset), turn_sem.at[chunk, 0])

    def turn_y(chunk):
        _, to_y, _, _, _, _, _, _, place_z, _, _, _ = route(chunk)
        return transfer(chunk, place_z, SHARDS + 1, TURN_BASE + 1, to_y, turn_sem.at[chunk, 1])

    def turn_x(chunk):
        _, _, to_x, _, _, _, _, _, _, place_y, _, slot_x = route(chunk)
        return transfer(chunk, place_y, slot_x, TURN_BASE + 2, to_x, turn_sem.at[chunk, 2])

    def begin(chunk):
        send(chunk, col, col, ROW_BASE + PAIR, near)
        send(chunk, col, col, ROW_BASE + LEFT, along_x(1))
        send(chunk, col, col, ROW_BASE + RIGHT, along_x(3))
        send(chunk, col, col, CORE_OWN, twin)

    def turn_first(chunk):
        for copy in load(chunk):
            copy.wait()
        moved_z = route(chunk)[3]
        pl.when(moved_z)(lambda: turn_z(chunk).start())

    def turn_second(chunk):
        _, _, _, moved_z, goes_y, _, _, _, _, _, _, _ = route(chunk)
        pl.when(moved_z)(lambda: turn_z(chunk).wait_recv())
        pl.when(goes_y)(lambda: turn_y(chunk).start())

    def turn_third(chunk):
        _, _, _, _, _, came_y, goes_x, _, _, _, _, _ = route(chunk)
        pl.when(came_y)(lambda: turn_y(chunk).wait_recv())
        pl.when(goes_x)(lambda: turn_x(chunk).start())

    def turned(chunk):
        _, _, _, _, _, _, _, came_x, _, _, place_x, _ = route(chunk)
        own_column = column_slot(chunk, 0, 0)
        pl.when(came_x)(lambda: arrived(chunk, own_column, TURN_BASE + 2))
        send(chunk, place_x, own_column, COLUMN_BASE + PAIR, across)
        send(chunk, place_x, own_column, COLUMN_BASE + LEFT, along_z(1))
        send(chunk, place_x, own_column, COLUMN_BASE + RIGHT, along_z(3))

    def relay(chunk, slot, base, event, forward, half=None):
        arrived(chunk, slot, base + event, half)
        for next_event, peer, next_half in forward:
            send(chunk, slot, slot, base + next_event, peer, next_half)
        if base == ROW_BASE:
            send(chunk, slot, slot, CORE_BASE + event, twin, half)

    def row_place(chunk, step, flip):
        return row_slot(step, flip, c)

    planes = ((ROW_BASE, row_place, along_x), (COLUMN_BASE, column_slot, along_z))

    def first(plane, chunk):
        base, slot, along = plane
        relay(chunk, slot(chunk, 0, 1), base, PAIR, ((PAIR_LEFT, along(1), None), (PAIR_RIGHT, along(3), None)))
        relay(chunk, slot(chunk, 3, 0), base, LEFT, ((LEFT_FAR, along(1), 0),))
        relay(chunk, slot(chunk, 1, 0), base, RIGHT, ((RIGHT_FAR, along(3), 1),))

    def second(plane, chunk):
        base, slot, along = plane
        if base in (COLUMN_BASE,):
            over = across if base == COLUMN_BASE else near
            relay(chunk, slot(chunk, 2, 0), base, LEFT_FAR, ((PAIR_LEFT_FAR, over, 0),), 0)
            relay(chunk, slot(chunk, 2, 0), base, RIGHT_FAR, ((PAIR_RIGHT_FAR, over, 1),), 1)
            relay(chunk, slot(chunk, 3, 1), base, PAIR_LEFT, ())
            relay(chunk, slot(chunk, 1, 1), base, PAIR_RIGHT, ())
        else:
            relay(chunk, slot(chunk, 3, 1), base, PAIR_LEFT, ((PAIR_LEFT_FAR, along(1), 0),))
            relay(chunk, slot(chunk, 1, 1), base, PAIR_RIGHT, ((PAIR_RIGHT_FAR, along(3), 1),))
            relay(chunk, slot(chunk, 2, 0), base, LEFT_FAR, (), 0)
            relay(chunk, slot(chunk, 2, 0), base, RIGHT_FAR, (), 1)

    def third(plane, chunk):
        base, slot, along = plane
        relay(chunk, slot(chunk, 2, 1), base, PAIR_LEFT_FAR, (), 0)
        relay(chunk, slot(chunk, 2, 1), base, PAIR_RIGHT_FAR, (), 1)

    row_first, column_first = functools.partial(first, planes[0]), functools.partial(first, planes[1])
    row_second, column_second = functools.partial(second, planes[0]), functools.partial(second, planes[1])
    row_third, column_third = functools.partial(third, planes[0]), functools.partial(third, planes[1])

    def from_twin(chunk):
        arrived(chunk, row_slot(0, 0, 1 - c), CORE_OWN)
        for step, flip, event, half in (
            (0, 1, PAIR, None), (3, 0, LEFT, None), (1, 0, RIGHT, None), (3, 1, PAIR_LEFT, None), (1, 1, PAIR_RIGHT, None),
            (2, 0, LEFT_FAR, 0), (2, 0, RIGHT_FAR, 1), (2, 1, PAIR_LEFT_FAR, 0), (2, 1, PAIR_RIGHT_FAR, 1),
        ):
            arrived(chunk, row_slot(step, flip, 1 - c), CORE_BASE + event, half)

    def split(chunk):
        own_column, place_x = column_slot(chunk, 0, 0), route(chunk)[10]

        @pl.loop(0, SHARDS)
        def _(shard):
            values = land[chunk, jnp.where(shard == own_column, place_x, shard)]
            leading = values.astype(jnp.bfloat16)
            trailing = (values - leading.astype(jnp.float32)).astype(jnp.bfloat16)
            where = pl.ds(pl.multiple_of(shard * rows, rows), rows)
            high[:, where, :] = leading
            low[:, where, :] = trailing

    rows_out = ROW_SHARDS * rows

    def multiply(k):
        ours, theirs = slice(0, rows_out), slice(rows_out, SHARDS * rows)
        o = perturbations
        left_side = jnp.concatenate(
            [high[k, ours], high[k, ours], low[k, ours], high[o, ours], low[o, ours], high[o, ours]], axis=1
        )
        right_side = jnp.concatenate(
            [high[o, theirs], low[o, theirs], high[o, theirs], high[k, theirs], high[k, theirs], low[k, theirs]], axis=1
        )
        total[k] += lax.dot_general(
            left_side, right_side, (((1,), (1,)), ((), ())), preferred_element_type=jnp.float32
        )

    def ahead(chunk, step):
        pl.when(chunk < chunks)(lambda: step(chunk))

    pl.semaphore_wait(barrier, len(peers))
    for chunk in range(3):
        turn_first(chunk)
    begin(0)

    @pl.loop(3, chunks)
    def _(chunk):
        turn_first(chunk)

    turn_second(0)
    turn_second(1)
    begin(1)
    turn_second(2)
    turn_third(0)
    row_first(0)
    turn_second(3)
    turn_third(1)
    turned(0)
    begin(2)

    @pl.loop(0, perturbations)
    def _(k):
        total[k] = jnp.zeros(total.shape[1:], jnp.float32)

    row_second(0)
    row_first(1)
    turn_second(4)
    turn_third(2)
    turned(1)
    begin(3)
    column_first(0)
    turn_second(5)
    turn_third(3)
    turned(2)
    column_second(0)
    column_first(1)

    @pl.loop(0, chunks)
    def _(chunk):
        ahead(chunk + 4, begin)
        ahead(chunk + 4, turn_third)
        ahead(chunk + 3, turned)
        ahead(chunk + 1, row_second)
        ahead(chunk + 2, row_first)
        ahead(chunk + 6, turn_second)
        ahead(chunk + 1, column_second)
        ahead(chunk + 2, column_first)
        row_third(chunk)
        column_third(chunk)
        from_twin(chunk)
        split(chunk)

        @pl.when(chunk < chunks - 1)
        def _():
            @pl.loop(0, perturbations)
            def _(k):
                multiply(k)

    @pl.loop(0, chunks)
    def _(chunk):
        sent = land.at[chunk, pl.ds(0, 22)]
        pltpu.make_async_copy(sent, sent, send_sem.at[chunk]).wait()
        _, _, _, moved_z, goes_y, _, goes_x, _, _, _, _, _ = route(chunk)
        pl.when(moved_z)(lambda: turn_z(chunk).wait_send())
        pl.when(goes_y)(lambda: turn_y(chunk).wait_send())
        pl.when(goes_x)(lambda: turn_x(chunk).wait_send())


def finish(high, low, total, density_ref):
    k, m = pl.program_id(0), pl.program_id(1)
    o = high.shape[0] - 1
    height, width = density_ref.shape[1:]
    ours = pl.ds(pl.multiple_of(m * height, height), height)
    theirs = slice(high.shape[1] - width, high.shape[1])
    left_side = jnp.concatenate(
        [high[k, ours], high[k, ours], low[k, ours], high[o, ours], low[o, ours], high[o, ours]], axis=1
    )
    right_side = jnp.concatenate(
        [high[o, theirs], low[o, theirs], high[o, theirs], high[k, theirs], high[k, theirs], low[k, theirs]], axis=1
    )
    density_ref[0] = total[k, ours] + lax.dot_general(
        left_side, right_side, (((1,), (1,)), ((), ())), preferred_element_type=jnp.float32
    )


def shards(response_coeffs, occupied_coeffs):
    perturbations, rows, occupied = response_coeffs.shape
    depth = occupied // CHUNKS
    height, width = ROW_SHARDS * rows, COLUMN_SHARDS * rows
    slices = (perturbations + 1, SHARDS * rows, depth)
    high, low, total = pl.pallas_call(
        kernel,
        name="gather_multiply",
        out_shape=[
            pltpu.VMEM(slices, jnp.bfloat16),
            pltpu.VMEM(slices, jnp.bfloat16),
            pltpu.VMEM((perturbations, height, width), jnp.float32),
        ],
        in_specs=[pl.BlockSpec(memory_space=pltpu.HBM)] * 2,
        out_specs=[pl.BlockSpec(memory_space=pltpu.VMEM)] * 3,
        scratch_shapes=[
            pltpu.VMEM((CHUNKS, SHARDS + TURN_SLOTS, perturbations + 1, rows, depth), jnp.float32),
            pltpu.SemaphoreType.DMA((CHUNKS, 2)),
            pltpu.SemaphoreType.DMA((CHUNKS,)),
            pltpu.SemaphoreType.DMA((CHUNKS, 3)),
            pltpu.SemaphoreType.DMA((CHUNKS, EVENTS)),
        ],
        compiler_params=pltpu.CompilerParams(
            collective_id=0, has_side_effects=True, vmem_limit_bytes=57475072
        ),
    )(response_coeffs, occupied_coeffs)
    tile = 1024
    return pl.pallas_call(
        finish,
        name="finish",
        grid=(perturbations, height // tile),
        out_shape=jax.ShapeDtypeStruct((perturbations, height, width), jnp.float32),
        in_specs=[pl.BlockSpec(memory_space=pltpu.VMEM)] * 3,
        out_specs=pl.BlockSpec((1, tile, width), lambda k, m: (k, m, 0)),
        compiler_params=pltpu.CompilerParams(vmem_limit_bytes=40 * 1024 * 1024),
    )(high, low, total)


def solution(mesh):
    return jax.shard_map(
        shards,
        mesh=mesh,
        in_specs=(P(None, ("row", "col"), None), P(("row", "col"), None)),
        out_specs=P(None, "row", "col"),
        check_vma=False,
    )
```

```python
import functools

import jax
import jax.numpy as jnp
from jax import lax
from jax.experimental import pallas as pl
from jax.experimental.pallas import tpu as pltpu
from jax.sharding import PartitionSpec as P

MESH = pl.DeviceIdType.MESH
CHUNKS = 8
ROW_SHARDS = 16
COLUMN_SHARDS = 8
SHARDS = ROW_SHARDS + COLUMN_SHARDS
TURN_SLOTS = 2

LEFT, RIGHT, PAIR, LEFT_FAR, RIGHT_FAR = 0, 1, 2, 3, 4
PAIR_LEFT, PAIR_RIGHT, PAIR_LEFT_FAR, PAIR_RIGHT_FAR = 5, 6, 7, 8
PLANE_EVENTS = 9
ROW_BASE = 0
COLUMN_BASE = PLANE_EVENTS
CORE_BASE = 2 * PLANE_EVENTS
CORE_OWN = 3 * PLANE_EVENTS
TURN_BASE = CORE_OWN + 1
EVENTS = TURN_BASE + 3
CROSSED = {ROW_BASE: (4, ()), COLUMN_BASE: (4, (0, 2))}


def kernel(response_ref, occupied_ref, high, low, total, land, load_sem, send_sem, turn_sem, recv_sem):
    perturbations, rows, occupied = response_ref.shape
    chunks, _, arrays, _, depth = land.shape
    row, col = lax.axis_index("row"), lax.axis_index("col")
    h, z = row // 4, row % 4
    x, l, c = col // 4, (col // 2) % 2, col % 2

    def device(h_, z_, x_, l_, c_):
        return (h_ * 4 + z_ % 4, (x_ % 4) * 4 + l_ * 2 + c_)

    def along_x(step):
        return device(h, z, x + step, l, c)

    def along_z(step):
        return device(h, z + step, x, l, c)

    near = device(h, z, x, 1 - l, c)
    across = device(1 - h, z, x, l, c)
    twin = device(h, z, x, l, 1 - c)

    def differs(a, b):
        return jnp.logical_or(a[0] != b[0], a[1] != b[1])

    here = device(h, z, x, l, c)
    h_s, z_s = x // 2, (x % 2) * 2 + l

    def route(chunk):
        odd = chunk % 2
        offset = (2 * c + l + 2 * odd) % 4
        to_y = device((h + x + odd) % 2, z, x, (z + offset) % 2, c)
        l_y = (z + l) % 2
        z_y = (z + 8 - 2 * c - l_y - 2 * odd) % 4
        h_y = (h + x + odd) % 2
        from_y = device(h_y, z, x, l_y, c)
        to_x = device(h, z, h_y * 2 + z_y // 2, l, x // 2)
        from_x = device(h, z, c * 2 + (h + h_s + odd) % 2, l, (z + 8 - z_s - 2 * odd) % 4 // 2)
        moved_z, came_y, came_x = offset != 0, differs(here, from_y), differs(here, from_x)
        goes_y, goes_x = differs(here, to_y), differs(here, to_x)
        place_z = jnp.where(moved_z, SHARDS, col)
        place_y = jnp.where(came_y, SHARDS + 1, place_z)
        place_x = jnp.where(came_x, column_slot(chunk, 0, 0), place_y)
        slot_x = ROW_SHARDS + (x % 2) * 4 + l_y * 2 + c
        return offset, to_y, to_x, moved_z, goes_y, came_y, goes_x, came_x, place_z, place_y, place_x, slot_x

    def column_slot(chunk, step, flip):
        odd = chunk % 2
        there = (z + step + 8 - z_s - 2 * odd) % 4
        return ROW_SHARDS + ((h + flip + h_s + odd) % 2) * 4 + (there % 2) * 2 + there // 2

    def row_slot(step, flip, core):
        return ((x + step) % 4) * 4 + ((l + flip) % 2) * 2 + core

    barrier = pltpu.get_barrier_semaphore()
    peers = [along_x(1), along_x(3), along_z(1), along_z(3), along_z(2)] + [near, across, twin]
    peers += [device(1 - h, z, x, 1 - l, c)] + [device(h, z, x + s, l, 1 - c) for s in (1, 2, 3)] + [along_x(2)]
    for peer in peers:
        pl.semaphore_signal(barrier, inc=1, device_id=peer, device_id_type=MESH)

    def load(chunk):
        columns = pl.ds(pl.multiple_of(chunk * depth, depth), depth)
        return (
            pltpu.make_async_copy(response_ref.at[:, :, columns], land.at[chunk, col, pl.ds(0, perturbations)], load_sem.at[chunk, 0]),
            pltpu.make_async_copy(occupied_ref.at[:, columns], land.at[chunk, col, perturbations], load_sem.at[chunk, 1]),
        )

    @pl.loop(0, chunks)
    def _(chunk):
        for copy in load(chunk):
            copy.start()

    def part(chunk, slot, half):
        if half is None:
            return land.at[chunk, slot]
        return land.at[chunk, slot, pl.ds(half * (arrays // 2), arrays // 2)]

    def transfer(chunk, source, slot, event, peer, sem=None, half=None):
        return pltpu.make_async_remote_copy(
            src_ref=part(chunk, source, half),
            dst_ref=part(chunk, slot, half),
            send_sem=send_sem.at[chunk] if sem is None else sem,
            recv_sem=recv_sem.at[chunk, event],
            device_id=peer,
            device_id_type=MESH,
        )

    def send(chunk, source, slot, event, peer, half=None):
        transfer(chunk, source, slot, event, peer, None, half).start()

    def arrived(chunk, slot, event, half=None):
        transfer(chunk, slot, slot, event, twin, None, half).wait_recv()

    def turn_z(chunk):
        offset = route(chunk)[0]
        return transfer(chunk, col, SHARDS, TURN_BASE, along_z(offset), turn_sem.at[chunk, 0])

    def turn_y(chunk):
        _, to_y, _, _, _, _, _, _, place_z, _, _, _ = route(chunk)
        return transfer(chunk, place_z, SHARDS + 1, TURN_BASE + 1, to_y, turn_sem.at[chunk, 1])

    def turn_x(chunk):
        _, _, to_x, _, _, _, _, _, _, place_y, _, slot_x = route(chunk)
        return transfer(chunk, place_y, slot_x, TURN_BASE + 2, to_x, turn_sem.at[chunk, 2])

    def begin(chunk):
        send(chunk, col, col, ROW_BASE + PAIR, near)
        send(chunk, col, col, ROW_BASE + LEFT, along_x(1))
        send(chunk, col, col, ROW_BASE + RIGHT, along_x(3))
        send(chunk, col, col, CORE_OWN, twin)

    def turn_first(chunk):
        for copy in load(chunk):
            copy.wait()
        moved_z = route(chunk)[3]
        pl.when(moved_z)(lambda: turn_z(chunk).start())

    def turn_second(chunk):
        _, _, _, moved_z, goes_y, _, _, _, _, _, _, _ = route(chunk)
        pl.when(moved_z)(lambda: turn_z(chunk).wait_recv())
        pl.when(goes_y)(lambda: turn_y(chunk).start())

    def turn_third(chunk):
        _, _, _, _, _, came_y, goes_x, _, _, _, _, _ = route(chunk)
        pl.when(came_y)(lambda: turn_y(chunk).wait_recv())
        pl.when(goes_x)(lambda: turn_x(chunk).start())

    def turned(chunk):
        _, _, _, _, _, _, _, came_x, _, _, place_x, _ = route(chunk)
        own_column = column_slot(chunk, 0, 0)
        pl.when(came_x)(lambda: arrived(chunk, own_column, TURN_BASE + 2))
        send(chunk, place_x, own_column, COLUMN_BASE + PAIR, across)
        send(chunk, place_x, own_column, COLUMN_BASE + LEFT, along_z(1))
        send(chunk, place_x, own_column, COLUMN_BASE + RIGHT, along_z(3))

    def relay(chunk, slot, base, event, forward, half=None):
        arrived(chunk, slot, base + event, half)
        for next_event, peer, next_half in forward:
            send(chunk, slot, slot, base + next_event, peer, next_half)
        if base == ROW_BASE:
            send(chunk, slot, slot, CORE_BASE + event, twin, half)

    def row_place(chunk, step, flip):
        return row_slot(step, flip, c)

    planes = ((ROW_BASE, row_place, along_x), (COLUMN_BASE, column_slot, along_z))

    def first(plane, chunk):
        base, slot, along = plane
        relay(chunk, slot(chunk, 0, 1), base, PAIR, ((PAIR_LEFT, along(1), None), (PAIR_RIGHT, along(3), None)))
        relay(chunk, slot(chunk, 3, 0), base, LEFT, ((LEFT_FAR, along(1), 0),))
        relay(chunk, slot(chunk, 1, 0), base, RIGHT, ((RIGHT_FAR, along(3), 1),))

    def second(plane, chunk):
        base, slot, along = plane
        over = near if base == ROW_BASE else across
        period, crossed_ones = CROSSED[base]
        crossed = functools.reduce(jnp.logical_or, [chunk % period == one for one in crossed_ones], False)

        def forward(when, slot_, event, peer, half):
            pl.when(when)(lambda: send(chunk, slot_, slot_, base + event, peer, half))

        relay(chunk, slot(chunk, 3, 1), base, PAIR_LEFT, ())
        forward(jnp.logical_not(crossed), slot(chunk, 3, 1), PAIR_LEFT_FAR, along(1), 0)
        relay(chunk, slot(chunk, 1, 1), base, PAIR_RIGHT, ())
        forward(jnp.logical_not(crossed), slot(chunk, 1, 1), PAIR_RIGHT_FAR, along(3), 1)
        relay(chunk, slot(chunk, 2, 0), base, LEFT_FAR, (), 0)
        forward(crossed, slot(chunk, 2, 0), PAIR_LEFT_FAR, over, 0)
        relay(chunk, slot(chunk, 2, 0), base, RIGHT_FAR, (), 1)
        forward(crossed, slot(chunk, 2, 0), PAIR_RIGHT_FAR, over, 1)

    def third(plane, chunk):
        base, slot, along = plane
        relay(chunk, slot(chunk, 2, 1), base, PAIR_LEFT_FAR, (), 0)
        relay(chunk, slot(chunk, 2, 1), base, PAIR_RIGHT_FAR, (), 1)

    row_first, column_first = functools.partial(first, planes[0]), functools.partial(first, planes[1])
    row_second, column_second = functools.partial(second, planes[0]), functools.partial(second, planes[1])
    row_third, column_third = functools.partial(third, planes[0]), functools.partial(third, planes[1])

    def from_twin(chunk):
        arrived(chunk, row_slot(0, 0, 1 - c), CORE_OWN)
        for step, flip, event, half in (
            (0, 1, PAIR, None), (3, 0, LEFT, None), (1, 0, RIGHT, None), (3, 1, PAIR_LEFT, None), (1, 1, PAIR_RIGHT, None),
            (2, 0, LEFT_FAR, 0), (2, 0, RIGHT_FAR, 1), (2, 1, PAIR_LEFT_FAR, 0), (2, 1, PAIR_RIGHT_FAR, 1),
        ):
            arrived(chunk, row_slot(step, flip, 1 - c), CORE_BASE + event, half)

    def split(chunk):
        own_column, place_x = column_slot(chunk, 0, 0), route(chunk)[10]

        @pl.loop(0, SHARDS)
        def _(shard):
            values = land[chunk, jnp.where(shard == own_column, place_x, shard)]
            leading = values.astype(jnp.bfloat16)
            trailing = (values - leading.astype(jnp.float32)).astype(jnp.bfloat16)
            where = pl.ds(pl.multiple_of(shard * rows, rows), rows)
            high[:, where, :] = leading
            low[:, where, :] = trailing

    rows_out = ROW_SHARDS * rows

    def multiply(k):
        ours, theirs = slice(0, rows_out), slice(rows_out, SHARDS * rows)
        o = perturbations
        left_side = jnp.concatenate(
            [high[k, ours], high[k, ours], low[k, ours], high[o, ours], low[o, ours], high[o, ours]], axis=1
        )
        right_side = jnp.concatenate(
            [high[o, theirs], low[o, theirs], high[o, theirs], high[k, theirs], high[k, theirs], low[k, theirs]], axis=1
        )
        total[k] += lax.dot_general(
            left_side, right_side, (((1,), (1,)), ((), ())), preferred_element_type=jnp.float32
        )

    def ahead(chunk, step):
        pl.when(chunk < chunks)(lambda: step(chunk))

    @pl.loop(0, perturbations)
    def _(k):
        total[k] = jnp.zeros(total.shape[1:], jnp.float32)

    pl.semaphore_wait(barrier, len(peers))
    for chunk in range(3):
        turn_first(chunk)
    begin(0)

    @pl.loop(3, chunks)
    def _(chunk):
        turn_first(chunk)

    turn_second(0)
    begin(1)
    turn_second(1)
    turn_third(0)
    turn_second(2)
    row_first(0)
    turned(0)
    turn_third(1)
    begin(2)

    turn_second(3)
    turn_third(2)
    turned(1)
    row_second(0)
    row_first(1)
    column_first(0)
    turn_second(4)
    turn_third(3)
    turned(2)
    begin(3)
    turn_second(5)
    column_second(0)
    column_first(1)

    @pl.loop(0, chunks)
    def _(chunk):
        ahead(chunk + 4, begin)
        ahead(chunk + 4, turn_third)
        ahead(chunk + 3, turned)
        ahead(chunk + 1, row_second)
        ahead(chunk + 2, row_first)
        ahead(chunk + 6, turn_second)
        ahead(chunk + 1, column_second)
        ahead(chunk + 2, column_first)
        row_third(chunk)
        column_third(chunk)
        from_twin(chunk)
        split(chunk)

        @pl.when(chunk < chunks - 1)
        def _():
            @pl.loop(0, perturbations)
            def _(k):
                multiply(k)

    @pl.loop(0, chunks)
    def _(chunk):
        sent = land.at[chunk, pl.ds(0, 22)]
        pltpu.make_async_copy(sent, sent, send_sem.at[chunk]).wait()
        _, _, _, moved_z, goes_y, _, goes_x, _, _, _, _, _ = route(chunk)
        pl.when(moved_z)(lambda: turn_z(chunk).wait_send())
        pl.when(goes_y)(lambda: turn_y(chunk).wait_send())
        pl.when(goes_x)(lambda: turn_x(chunk).wait_send())


def finish(high, low, total, density_ref):
    k, m = pl.program_id(0), pl.program_id(1)
    o = high.shape[0] - 1
    height, width = density_ref.shape[1:]
    ours = pl.ds(pl.multiple_of(m * height, height), height)
    theirs = slice(high.shape[1] - width, high.shape[1])
    left_side = jnp.concatenate(
        [high[k, ours], high[k, ours], low[k, ours], high[o, ours], low[o, ours], high[o, ours]], axis=1
    )
    right_side = jnp.concatenate(
        [high[o, theirs], low[o, theirs], high[o, theirs], high[k, theirs], high[k, theirs], low[k, theirs]], axis=1
    )
    density_ref[0] = total[k, ours] + lax.dot_general(
        left_side, right_side, (((1,), (1,)), ((), ())), preferred_element_type=jnp.float32
    )


def shards(response_coeffs, occupied_coeffs):
    perturbations, rows, occupied = response_coeffs.shape
    depth = occupied // CHUNKS
    height, width = ROW_SHARDS * rows, COLUMN_SHARDS * rows
    slices = (perturbations + 1, SHARDS * rows, depth)
    high, low, total = pl.pallas_call(
        kernel,
        name="gather_multiply",
        out_shape=[
            pltpu.VMEM(slices, jnp.bfloat16),
            pltpu.VMEM(slices, jnp.bfloat16),
            pltpu.VMEM((perturbations, height, width), jnp.float32),
        ],
        in_specs=[pl.BlockSpec(memory_space=pltpu.HBM)] * 2,
        out_specs=[pl.BlockSpec(memory_space=pltpu.VMEM)] * 3,
        scratch_shapes=[
            pltpu.VMEM((CHUNKS, SHARDS + TURN_SLOTS, perturbations + 1, rows, depth), jnp.float32),
            pltpu.SemaphoreType.DMA((CHUNKS, 2)),
            pltpu.SemaphoreType.DMA((CHUNKS,)),
            pltpu.SemaphoreType.DMA((CHUNKS, 3)),
            pltpu.SemaphoreType.DMA((CHUNKS, EVENTS)),
        ],
        compiler_params=pltpu.CompilerParams(
            collective_id=0, has_side_effects=True, vmem_limit_bytes=57475072
        ),
    )(response_coeffs, occupied_coeffs)
    tile = 1024
    return pl.pallas_call(
        finish,
        name="finish",
        grid=(perturbations, height // tile),
        out_shape=jax.ShapeDtypeStruct((perturbations, height, width), jnp.float32),
        in_specs=[pl.BlockSpec(memory_space=pltpu.VMEM)] * 3,
        out_specs=pl.BlockSpec((1, tile, width), lambda k, m: (k, m, 0)),
        compiler_params=pltpu.CompilerParams(vmem_limit_bytes=40 * 1024 * 1024),
    )(high, low, total)


def solution(mesh):
    return jax.shard_map(
        shards,
        mesh=mesh,
        in_specs=(P(None, ("row", "col"), None), P(("row", "col"), None)),
        out_specs=P(None, "row", "col"),
        check_vma=False,
    )
```

```python
import functools

import jax
import jax.numpy as jnp
from jax import lax
from jax.experimental import pallas as pl
from jax.experimental.pallas import tpu as pltpu
from jax.sharding import PartitionSpec as P

MESH = pl.DeviceIdType.MESH
CHUNKS = 8
ROW_SHARDS = 16
COLUMN_SHARDS = 8
SHARDS = ROW_SHARDS + COLUMN_SHARDS
TURN_SLOTS = 2

LEFT, RIGHT, PAIR, LEFT_FAR, RIGHT_FAR = 0, 1, 2, 3, 4
PAIR_LEFT, PAIR_RIGHT, PAIR_LEFT_FAR, PAIR_RIGHT_FAR = 5, 6, 7, 8
PLANE_EVENTS = 9
ROW_BASE = 0
COLUMN_BASE = PLANE_EVENTS
CORE_BASE = 2 * PLANE_EVENTS
CORE_OWN = 3 * PLANE_EVENTS
TURN_BASE = CORE_OWN + 1
EVENTS = TURN_BASE + 3
CROSSED = {ROW_BASE: (4, ()), COLUMN_BASE: (4, (0, 2))}


def kernel(response_ref, occupied_ref, high, low, total, land, load_sem, send_sem, turn_sem, recv_sem):
    perturbations, rows, occupied = response_ref.shape
    chunks, _, arrays, _, depth = land.shape
    row, col = lax.axis_index("row"), lax.axis_index("col")
    h, z = row // 4, row % 4
    x, l, c = col // 4, (col // 2) % 2, col % 2

    def device(h_, z_, x_, l_, c_):
        return (h_ * 4 + z_ % 4, (x_ % 4) * 4 + l_ * 2 + c_)

    def along_x(step):
        return device(h, z, x + step, l, c)

    def along_z(step):
        return device(h, z + step, x, l, c)

    near = device(h, z, x, 1 - l, c)
    across = device(1 - h, z, x, l, c)
    twin = device(h, z, x, l, 1 - c)

    def differs(a, b):
        return jnp.logical_or(a[0] != b[0], a[1] != b[1])

    here = device(h, z, x, l, c)
    h_s, z_s = x // 2, (x % 2) * 2 + l

    def route(chunk):
        odd = chunk % 2
        offset = (2 * c + l + 2 * odd) % 4
        to_y = device((h + x + odd) % 2, z, x, (z + offset) % 2, c)
        l_y = (z + l) % 2
        z_y = (z + 8 - 2 * c - l_y - 2 * odd) % 4
        h_y = (h + x + odd) % 2
        from_y = device(h_y, z, x, l_y, c)
        to_x = device(h, z, h_y * 2 + z_y // 2, l, x // 2)
        from_x = device(h, z, c * 2 + (h + h_s + odd) % 2, l, (z + 8 - z_s - 2 * odd) % 4 // 2)
        moved_z, came_y, came_x = offset != 0, differs(here, from_y), differs(here, from_x)
        goes_y, goes_x = differs(here, to_y), differs(here, to_x)
        place_z = jnp.where(moved_z, SHARDS, col)
        place_y = jnp.where(came_y, SHARDS + 1, place_z)
        place_x = jnp.where(came_x, column_slot(chunk, 0, 0), place_y)
        slot_x = ROW_SHARDS + (x % 2) * 4 + l_y * 2 + c
        return offset, to_y, to_x, moved_z, goes_y, came_y, goes_x, came_x, place_z, place_y, place_x, slot_x

    def column_slot(chunk, step, flip):
        odd = chunk % 2
        there = (z + step + 8 - z_s - 2 * odd) % 4
        return ROW_SHARDS + ((h + flip + h_s + odd) % 2) * 4 + (there % 2) * 2 + there // 2

    def row_slot(step, flip, core):
        return ((x + step) % 4) * 4 + ((l + flip) % 2) * 2 + core

    barrier = pltpu.get_barrier_semaphore()
    peers = [along_x(1), along_x(3), along_z(1), along_z(3), along_z(2)] + [near, across, twin]
    peers += [device(1 - h, z, x, 1 - l, c)] + [device(h, z, x + s, l, 1 - c) for s in (1, 2, 3)] + [along_x(2)]
    for peer in peers:
        pl.semaphore_signal(barrier, inc=1, device_id=peer, device_id_type=MESH)

    def load(chunk):
        columns = pl.ds(pl.multiple_of(chunk * depth, depth), depth)
        return (
            pltpu.make_async_copy(response_ref.at[:, :, columns], land.at[chunk, col, pl.ds(0, perturbations)], load_sem.at[chunk, 0]),
            pltpu.make_async_copy(occupied_ref.at[:, columns], land.at[chunk, col, perturbations], load_sem.at[chunk, 1]),
        )

    @pl.loop(0, chunks)
    def _(chunk):
        for copy in load(chunk):
            copy.start()

    def part(chunk, slot, half):
        if half is None:
            return land.at[chunk, slot]
        return land.at[chunk, slot, pl.ds(half * (arrays // 2), arrays // 2)]

    def transfer(chunk, source, slot, event, peer, sem=None, half=None):
        return pltpu.make_async_remote_copy(
            src_ref=part(chunk, source, half),
            dst_ref=part(chunk, slot, half),
            send_sem=send_sem.at[chunk] if sem is None else sem,
            recv_sem=recv_sem.at[chunk, event],
            device_id=peer,
            device_id_type=MESH,
        )

    def send(chunk, source, slot, event, peer, half=None):
        transfer(chunk, source, slot, event, peer, None, half).start()

    def arrived(chunk, slot, event, half=None):
        transfer(chunk, slot, slot, event, twin, None, half).wait_recv()

    def turn_z(chunk):
        offset = route(chunk)[0]
        return transfer(chunk, col, SHARDS, TURN_BASE, along_z(offset), turn_sem.at[chunk, 0])

    def turn_y(chunk):
        _, to_y, _, _, _, _, _, _, place_z, _, _, _ = route(chunk)
        return transfer(chunk, place_z, SHARDS + 1, TURN_BASE + 1, to_y, turn_sem.at[chunk, 1])

    def turn_x(chunk):
        _, _, to_x, _, _, _, _, _, _, place_y, _, slot_x = route(chunk)
        return transfer(chunk, place_y, slot_x, TURN_BASE + 2, to_x, turn_sem.at[chunk, 2])

    def begin(chunk):
        send(chunk, col, col, ROW_BASE + PAIR, near)
        send(chunk, col, col, ROW_BASE + LEFT, along_x(1))
        send(chunk, col, col, ROW_BASE + RIGHT, along_x(3))
        send(chunk, col, col, CORE_OWN, twin)

    def turn_first(chunk):
        for copy in load(chunk):
            copy.wait()
        moved_z = route(chunk)[3]
        pl.when(moved_z)(lambda: turn_z(chunk).start())

    def turn_second(chunk):
        _, _, _, moved_z, goes_y, _, _, _, _, _, _, _ = route(chunk)
        pl.when(moved_z)(lambda: turn_z(chunk).wait_recv())
        pl.when(goes_y)(lambda: turn_y(chunk).start())

    def turn_third(chunk):
        _, _, _, _, _, came_y, goes_x, _, _, _, _, _ = route(chunk)
        pl.when(came_y)(lambda: turn_y(chunk).wait_recv())
        pl.when(goes_x)(lambda: turn_x(chunk).start())

    def turned(chunk):
        _, _, _, _, _, _, _, came_x, _, _, place_x, _ = route(chunk)
        own_column = column_slot(chunk, 0, 0)
        pl.when(came_x)(lambda: arrived(chunk, own_column, TURN_BASE + 2))
        send(chunk, place_x, own_column, COLUMN_BASE + PAIR, across)
        send(chunk, place_x, own_column, COLUMN_BASE + LEFT, along_z(1))
        send(chunk, place_x, own_column, COLUMN_BASE + RIGHT, along_z(3))

    def relay(chunk, slot, base, event, forward, half=None):
        arrived(chunk, slot, base + event, half)
        for next_event, peer, next_half in forward:
            send(chunk, slot, slot, base + next_event, peer, next_half)
        if base == ROW_BASE:
            send(chunk, slot, slot, CORE_BASE + event, twin, half)

    def row_place(chunk, step, flip):
        return row_slot(step, flip, c)

    planes = ((ROW_BASE, row_place, along_x), (COLUMN_BASE, column_slot, along_z))

    def first(plane, chunk):
        base, slot, along = plane
        relay(chunk, slot(chunk, 0, 1), base, PAIR, ((PAIR_LEFT, along(1), None), (PAIR_RIGHT, along(3), None)))
        relay(chunk, slot(chunk, 3, 0), base, LEFT, ((LEFT_FAR, along(1), 0),))
        relay(chunk, slot(chunk, 1, 0), base, RIGHT, ((RIGHT_FAR, along(3), 1),))

    def second(plane, chunk):
        base, slot, along = plane
        over = near if base == ROW_BASE else across
        period, crossed_ones = CROSSED[base]
        crossed = functools.reduce(jnp.logical_or, [chunk % period == one for one in crossed_ones], False)

        def forward(when, slot_, event, peer, half):
            pl.when(when)(lambda: send(chunk, slot_, slot_, base + event, peer, half))

        relay(chunk, slot(chunk, 3, 1), base, PAIR_LEFT, ())
        forward(jnp.logical_not(crossed), slot(chunk, 3, 1), PAIR_LEFT_FAR, along(1), 0)
        relay(chunk, slot(chunk, 1, 1), base, PAIR_RIGHT, ())
        forward(jnp.logical_not(crossed), slot(chunk, 1, 1), PAIR_RIGHT_FAR, along(3), 1)
        relay(chunk, slot(chunk, 2, 0), base, LEFT_FAR, (), 0)
        forward(crossed, slot(chunk, 2, 0), PAIR_LEFT_FAR, over, 0)
        relay(chunk, slot(chunk, 2, 0), base, RIGHT_FAR, (), 1)
        forward(crossed, slot(chunk, 2, 0), PAIR_RIGHT_FAR, over, 1)

    def third(plane, chunk):
        base, slot, along = plane
        relay(chunk, slot(chunk, 2, 1), base, PAIR_LEFT_FAR, (), 0)
        relay(chunk, slot(chunk, 2, 1), base, PAIR_RIGHT_FAR, (), 1)

    row_first, column_first = functools.partial(first, planes[0]), functools.partial(first, planes[1])
    row_second, column_second = functools.partial(second, planes[0]), functools.partial(second, planes[1])
    row_third, column_third = functools.partial(third, planes[0]), functools.partial(third, planes[1])

    def from_twin(chunk):
        arrived(chunk, row_slot(0, 0, 1 - c), CORE_OWN)
        for step, flip, event, half in (
            (0, 1, PAIR, None), (3, 0, LEFT, None), (1, 0, RIGHT, None), (3, 1, PAIR_LEFT, None), (1, 1, PAIR_RIGHT, None),
            (2, 0, LEFT_FAR, 0), (2, 0, RIGHT_FAR, 1), (2, 1, PAIR_LEFT_FAR, 0), (2, 1, PAIR_RIGHT_FAR, 1),
        ):
            arrived(chunk, row_slot(step, flip, 1 - c), CORE_BASE + event, half)

    def split(chunk):
        own_column, place_x = column_slot(chunk, 0, 0), route(chunk)[10]

        @pl.loop(0, SHARDS)
        def _(shard):
            values = land[chunk, jnp.where(shard == own_column, place_x, shard)]
            leading = values.astype(jnp.bfloat16)
            trailing = (values - leading.astype(jnp.float32)).astype(jnp.bfloat16)
            where = pl.ds(pl.multiple_of(shard * rows, rows), rows)
            high[:, where, :] = leading
            low[:, where, :] = trailing

    rows_out = ROW_SHARDS * rows

    def multiply(k):
        ours, theirs = slice(0, rows_out), slice(rows_out, SHARDS * rows)
        o = perturbations
        left_side = jnp.concatenate(
            [high[k, ours], high[k, ours], low[k, ours], high[o, ours], low[o, ours], high[o, ours]], axis=1
        )
        right_side = jnp.concatenate(
            [high[o, theirs], low[o, theirs], high[o, theirs], high[k, theirs], high[k, theirs], low[k, theirs]], axis=1
        )
        total[k] += lax.dot_general(
            left_side, right_side, (((1,), (1,)), ((), ())), preferred_element_type=jnp.float32
        )

    def ahead(chunk, step):
        pl.when(chunk < chunks)(lambda: step(chunk))

    @pl.loop(0, perturbations)
    def _(k):
        total[k] = jnp.zeros(total.shape[1:], jnp.float32)

    pl.semaphore_wait(barrier, len(peers))
    for chunk in range(3):
        turn_first(chunk)
    begin(0)

    @pl.loop(3, chunks)
    def _(chunk):
        turn_first(chunk)

    turn_second(0)
    begin(1)
    turn_second(1)
    turn_third(0)
    turn_second(2)
    row_first(0)
    turned(0)
    turn_third(1)
    begin(2)

    turn_second(3)
    turn_third(2)
    turned(1)
    row_second(0)
    row_first(1)
    column_first(0)
    turn_second(4)
    turn_third(3)
    turned(2)
    begin(3)
    turn_second(5)
    column_second(0)
    column_first(1)

    @pl.loop(0, chunks)
    def _(chunk):
        ahead(chunk + 4, begin)
        ahead(chunk + 4, turn_third)
        ahead(chunk + 3, turned)
        ahead(chunk + 1, row_second)
        ahead(chunk + 2, row_first)
        pl.when(chunk > 0)(lambda: multiply(0))
        ahead(chunk + 6, turn_second)
        ahead(chunk + 1, column_second)
        ahead(chunk + 2, column_first)
        pl.when(chunk > 0)(lambda: multiply(1))
        row_third(chunk)
        pl.when(chunk > 0)(lambda: multiply(2))
        column_third(chunk)
        from_twin(chunk)
        split(chunk)

    @pl.loop(0, chunks)
    def _(chunk):
        sent = land.at[chunk, pl.ds(0, 22)]
        pltpu.make_async_copy(sent, sent, send_sem.at[chunk]).wait()
        _, _, _, moved_z, goes_y, _, goes_x, _, _, _, _, _ = route(chunk)
        pl.when(moved_z)(lambda: turn_z(chunk).wait_send())
        pl.when(goes_y)(lambda: turn_y(chunk).wait_send())
        pl.when(goes_x)(lambda: turn_x(chunk).wait_send())


def finish(high, low, total, density_ref):
    k, m = pl.program_id(0), pl.program_id(1)
    o = high.shape[0] - 1
    height, width = density_ref.shape[1:]
    ours = pl.ds(pl.multiple_of(m * height, height), height)
    theirs = slice(high.shape[1] - width, high.shape[1])
    left_side = jnp.concatenate(
        [high[k, ours], high[k, ours], low[k, ours], high[o, ours], low[o, ours], high[o, ours]], axis=1
    )
    right_side = jnp.concatenate(
        [high[o, theirs], low[o, theirs], high[o, theirs], high[k, theirs], high[k, theirs], low[k, theirs]], axis=1
    )
    density_ref[0] = total[k, ours] + lax.dot_general(
        left_side, right_side, (((1,), (1,)), ((), ())), preferred_element_type=jnp.float32
    )


def shards(response_coeffs, occupied_coeffs):
    perturbations, rows, occupied = response_coeffs.shape
    depth = occupied // CHUNKS
    height, width = ROW_SHARDS * rows, COLUMN_SHARDS * rows
    slices = (perturbations + 1, SHARDS * rows, depth)
    high, low, total = pl.pallas_call(
        kernel,
        name="gather_multiply",
        out_shape=[
            pltpu.VMEM(slices, jnp.bfloat16),
            pltpu.VMEM(slices, jnp.bfloat16),
            pltpu.VMEM((perturbations, height, width), jnp.float32),
        ],
        in_specs=[pl.BlockSpec(memory_space=pltpu.HBM)] * 2,
        out_specs=[pl.BlockSpec(memory_space=pltpu.VMEM)] * 3,
        scratch_shapes=[
            pltpu.VMEM((CHUNKS, SHARDS + TURN_SLOTS, perturbations + 1, rows, depth), jnp.float32),
            pltpu.SemaphoreType.DMA((CHUNKS, 2)),
            pltpu.SemaphoreType.DMA((CHUNKS,)),
            pltpu.SemaphoreType.DMA((CHUNKS, 3)),
            pltpu.SemaphoreType.DMA((CHUNKS, EVENTS)),
        ],
        compiler_params=pltpu.CompilerParams(
            collective_id=0, has_side_effects=True, vmem_limit_bytes=57475072
        ),
    )(response_coeffs, occupied_coeffs)
    tile = 1024
    return pl.pallas_call(
        finish,
        name="finish",
        grid=(perturbations, height // tile),
        out_shape=jax.ShapeDtypeStruct((perturbations, height, width), jnp.float32),
        in_specs=[pl.BlockSpec(memory_space=pltpu.VMEM)] * 3,
        out_specs=pl.BlockSpec((1, tile, width), lambda k, m: (k, m, 0)),
        compiler_params=pltpu.CompilerParams(vmem_limit_bytes=40 * 1024 * 1024),
    )(high, low, total)


def solution(mesh):
    return jax.shard_map(
        shards,
        mesh=mesh,
        in_specs=(P(None, ("row", "col"), None), P(("row", "col"), None)),
        out_specs=P(None, "row", "col"),
        check_vma=False,
    )
```
